512 devices in a mesh: row: 16 (over z_lo, x), col: 32 (over y, z_hi, core).
Axes of the slice: x: 4, y: 4, z: 16 (z_hi: 4, z_lo: 4; z = z_hi * 4 + z_lo), core: 2. Of those that a mesh axis runs over, the one named last changes fastest.
Arguments:
- potential_temp: bfloat16 [64, 1024, 1024], P(None, 'col', 'row'), may hold values from -6 to 6
- humidity: bfloat16 [64, 1024, 1024], P(None, 'col', 'row'), may hold values from 0.099609375 to 1
- absorb: float32 [4, 64], replicated, may hold values from 0.002 to 0.2
- solar_flux: float32 [4], replicated, may hold values from 2 to 8
- emission: float32 [4], replicated, may hold values from 0.5 to 4
- sunlit: int32 [16, 32], replicated, may hold values from 0 to 2048
- project: float32 [32, 64], replicated, may hold values from -0.75 to 0.75
- restore: float32 [64, 32], replicated, may hold values from -1 to 1
- east_basis: bfloat16 [1024, 1024], replicated, may hold values from -0.1875 to 0.1875
- north_basis: bfloat16 [1024, 1024], replicated, may hold values from -0.1875 to 0.1875
- east_weight: float32 [1024], replicated, may hold values from 0.5 to 2
- north_weight: float32 [1024], replicated, may hold values from 0.5 to 2
- east_eigen: float32 [1024], replicated, may hold values from 0.05 to 4
- north_eigen: float32 [1024], replicated, may hold values from 0.05 to 4
- coupling: float32 [32], replicated, may hold values from 0.05 to 2
Outputs:
- new_state: bfloat16 [64, 1024, 1024], P(None, 'col', 'row')
The draws below stay inside these ranges and needn't reach their ends.
All inputs are finite; a program needn't handle non-finite values.
Results may differ from the reference program's by a relative error of at most 0.01.
Values may be sent and summed in bfloat16 or wider, within the bound.
No kernel may reach another device: no remote copies, remote signals or barrier semaphores. Data moves between devices by JAX's collectives and lax.ppermute only.
A program may use at most 64 MiB of HBM per device.

```python
import math
import jax
import jax.numpy as jnp
from jax import lax

NX = 1024
NY = 1024
L = 64
M = 32
BANDS = 4
TILE = 2048
N_ROW = 16
N_COL = 32


def place_ends(entries, stream_key, low, high):
    index_at = [jax.random.randint(jax.random.fold_in(stream_key, axis), (), 0, length) for axis, length in enumerate(entries.shape)]
    main_axis = entries.shape.index(max(entries.shape))
    next_to = index_at[:main_axis] + [(index_at[main_axis] + 1) % entries.shape[main_axis]] + index_at[main_axis + 1:]
    return entries.at[tuple(index_at)].set(low).at[tuple(next_to)].set(high)


def block_levels(stream_key, dims, split, smallest, top_value):
    def one(position, blocks):
        draws = jax.random.uniform(jax.random.fold_in(jax.random.fold_in(stream_key, 6), position), (blocks,), jnp.float32, smallest / len(split), top_value / len(split))
        return jnp.repeat(jnp.exp(draws), dims[position] // blocks).reshape((-1,) + (1,) * (len(dims) - position - 1))

    loudness = one(*split[0])
    for cut in split[1:]:
        loudness = loudness * one(*cut)
    return loudness


def centred(rng, extent, width, most, split=(), held_as=jnp.bfloat16):
    factor_of = block_levels(rng, extent, split, -0.22, 0.18) if split else 1.0
    result = jax.random.normal(rng, extent, jnp.float32) * width * factor_of
    return jnp.minimum(jnp.maximum(result, -most), most).astype(held_as)


def setup_inputs(seed: int = 0) -> dict:
    streams_of = jax.random.split(jax.random.key(seed), 16)
    return {
        "potential_temp": centred(streams_of[0], (L, NX, NY), 1.0, 6.0, ((1, 32), (2, 16))),
        "humidity": jnp.clip(0.099609375 + 0.9003906 * jax.random.uniform(streams_of[1], (L, NX, NY), jnp.float32) ** block_levels(streams_of[1], (L, NX, NY), ((1, 32), (2, 16)), -0.2, 0.2), 0.099609375, 1.0).astype(jnp.bfloat16),
        "absorb": jnp.clip(jnp.exp(jax.random.uniform(streams_of[2], (BANDS, L), jnp.float32, math.log(0.002), math.log(0.2))), 0.002, 0.2),
        "solar_flux": jnp.clip(jnp.exp(jax.random.uniform(streams_of[3], (BANDS,), jnp.float32, math.log(2.0), math.log(8.0))), 2.0, 8.0),
        "emission": jnp.clip(jnp.exp(jax.random.uniform(streams_of[4], (BANDS,), jnp.float32, math.log(0.5), math.log(4.0))), 0.5, 4.0),
        "sunlit": place_ends(jax.random.randint(streams_of[5], (N_ROW, N_COL), 0, TILE + 1), jax.random.fold_in(streams_of[5], 1), 0, TILE).astype(jnp.int32),
        "project": centred(streams_of[6], (M, L), L ** -0.5, 0.75, (), jnp.float32),
        "restore": centred(streams_of[7], (L, M), M ** -0.5, 1.0, (), jnp.float32),
        "east_basis": centred(streams_of[8], (NX, NX), NX ** -0.5, 0.1875),
        "north_basis": centred(streams_of[9], (NY, NY), NY ** -0.5, 0.1875),
        "east_weight": jnp.clip(jnp.exp(jax.random.uniform(streams_of[10], (NX,), jnp.float32, math.log(0.5), math.log(2.0))), 0.5, 2.0),
        "north_weight": jnp.clip(jnp.exp(jax.random.uniform(streams_of[11], (NY,), jnp.float32, math.log(0.5), math.log(2.0))), 0.5, 2.0),
        "east_eigen": jnp.clip(jnp.exp(jax.random.uniform(streams_of[12], (NX,), jnp.float32, math.log(0.05), math.log(4.0))), 0.05, 4.0),
        "north_eigen": jnp.clip(jnp.exp(jax.random.uniform(streams_of[13], (NY,), jnp.float32, math.log(0.05), math.log(4.0))), 0.05, 4.0),
        "coupling": jnp.clip(jnp.exp(jax.random.uniform(streams_of[14], (M,), jnp.float32, math.log(0.05), math.log(2.0))), 0.05, 2.0),
    }


def lower_triangle(levels):
    level_index = jnp.arange(levels, dtype=jnp.int32)
    return (level_index[:, None] >= level_index[None, :]).astype(jnp.float32)


def shortwave(vapour, absorb, solar_flux, triangle):
    heating = jnp.zeros(vapour.shape, jnp.float32)
    for band_index in range(absorb.shape[0]):
        optical = absorb[band_index][:, None] * vapour
        column_depth = jnp.dot(triangle, optical, precision=lax.Precision.HIGHEST, preferred_element_type=jnp.float32)
        heating = heating + solar_flux[band_index] * (jnp.exp(optical - column_depth) - jnp.exp(-column_depth))
    return heating


def longwave(column_temp, vapour, absorb, emission):
    cooling = jnp.zeros(vapour.shape, jnp.float32)
    for band_index in range(absorb.shape[0]):
        optical = absorb[band_index][:, None] * vapour
        cooling = cooling + emission[band_index] * (1.0 - jnp.exp(-optical)) * column_temp
    return cooling


def reference(potential_temp, humidity, absorb, solar_flux, emission, sunlit, project, restore, east_basis, north_basis, east_weight, north_weight, east_eigen, north_eigen, coupling):
    east_local = NX // N_COL
    north_local = NY // N_ROW
    east_index = jnp.arange(NX, dtype=jnp.int32)
    north_index = jnp.arange(NY, dtype=jnp.int32)
    within = (east_index % east_local)[:, None] * north_local + (north_index % north_local)[None, :]
    lit_count = sunlit[(north_index // north_local)[None, :], (east_index // east_local)[:, None]]
    mask = (within < lit_count).astype(jnp.float32).reshape(1, NX * NY)
    column_temp = potential_temp.astype(jnp.float32).reshape(L, NX * NY)
    vapour = humidity.astype(jnp.float32).reshape(L, NX * NY)
    triangle = lower_triangle(L)
    forcing = column_temp + shortwave(vapour, absorb, solar_flux, triangle) * mask - longwave(column_temp, vapour, absorb, emission)
    modal_field = jnp.dot(project, forcing, precision=lax.Precision.HIGHEST, preferred_element_type=jnp.float32).astype(jnp.bfloat16)
    modal_field = modal_field.reshape(M, NX, NY)
    east_scaled = (east_basis.astype(jnp.float32) * east_weight[:, None]).astype(jnp.bfloat16)
    north_scaled = (north_basis.astype(jnp.float32) * north_weight[:, None]).astype(jnp.bfloat16)
    spectral_east = jnp.einsum("xi,mxy->miy", east_scaled.astype(jnp.float32), modal_field.astype(jnp.float32), precision=lax.Precision.HIGHEST).astype(jnp.bfloat16)
    spectral = jnp.einsum("miy,yj->mij", spectral_east.astype(jnp.float32), north_scaled.astype(jnp.float32), precision=lax.Precision.HIGHEST)
    divisor = 1.0 + coupling[:, None, None] * (east_eigen[:, None] + north_eigen[None, :])[None]
    scaled = (spectral / divisor).astype(jnp.bfloat16)
    north_back = jnp.einsum("mij,yj->miy", scaled.astype(jnp.float32), north_basis.astype(jnp.float32), precision=lax.Precision.HIGHEST).astype(jnp.bfloat16)
    solved = jnp.einsum("xi,miy->mxy", east_basis.astype(jnp.float32), north_back.astype(jnp.float32), precision=lax.Precision.HIGHEST).astype(jnp.bfloat16)
    difference = solved.reshape(M, NX * NY).astype(jnp.float32) - modal_field.reshape(M, NX * NY).astype(jnp.float32)
    correction = jnp.dot(restore, difference, precision=lax.Precision.HIGHEST, preferred_element_type=jnp.float32)
    return (forcing + correction).astype(jnp.bfloat16).reshape(L, NX, NY)
```

```python
import jax
import jax.numpy as jnp
from jax import lax
from jax.experimental import pallas as pl
from jax.experimental.pallas import tpu as pltpu
from jax.sharding import PartitionSpec as P

F32 = jnp.float32
BF16 = jnp.bfloat16
HALF = 64
LANES = 128
VMEM_LIMIT = 12 * 1024 * 1024


def dot(a, b, da, db):
    return lax.dot_general(a, b, (((da,), (db,)), ((), ())), preferred_element_type=F32)


def fold(v):
    n = v.shape[0] // 2
    return jnp.concatenate([v[:n], v[n:]], axis=1)


def unfold(v):
    k, n, _ = v.shape
    return jnp.concatenate([v[:, :, :HALF], v[:, :, HALF:]], axis=1).reshape(k * 2 * n, HALF)


def halves(v):
    high = v.astype(BF16)
    return high, (v - high.astype(F32)).astype(BF16)


def left_terms(v):
    high, low = halves(v)
    return jnp.concatenate([high, low, high], axis=1)


def right_terms(v):
    high, low = halves(v)
    return jnp.concatenate([high, high, low], axis=0)


def column_of(row, first, rows, lane):
    place = lax.broadcasted_iota(jnp.int32, (rows, LANES), 0) + first
    return jnp.sum(jnp.where(lane == place, jnp.broadcast_to(row, (rows, LANES)), 0.0), axis=1, keepdims=True)


def physics(absorb, flux, emission, sunlit, temp, vapour, project, wx, wy, forcing, send, modal, scratch):
    levels = temp.shape[0]
    bands = absorb.shape[0]
    rows = temp.shape[1] // 2
    r = lax.axis_index("row")
    c = lax.axis_index("col")
    shape = (rows, LANES)
    lane = lax.broadcasted_iota(jnp.int32, shape, 1)
    upper = lane >= HALF
    number = lax.broadcasted_iota(jnp.int32, shape, 0) * HALF + lane + jnp.where(upper, rows * HALF - HALF, 0)
    lit = (number < sunlit[r, c]).astype(F32)
    through = [lit * flux[b] for b in range(bands)]
    before = through[0] + through[1] + through[2] + through[3]
    emitted = emission[0] + emission[1] + emission[2] + emission[3]
    for level in range(levels):
        t = fold(temp[level]).astype(F32)
        h = fold(vapour[level]).astype(F32)
        kept = None
        after = None
        for b in range(bands):
            pass_through = jnp.exp(h * (-absorb[b, level]))
            through[b] = through[b] * pass_through
            part = pass_through * emission[b]
            kept = part if kept is None else kept + part
            after = through[b] if after is None else after + through[b]
        forcing[level] = t + (before - after) - (emitted - kept) * t
        before = after
    left = left_terms(project[...])
    for p in range(0, rows, 2):
        field = jnp.concatenate([forcing[:, p, :], forcing[:, p + 1, :]], axis=1)
        out = dot(left, right_terms(field), 1, 0)
        scratch[:, p, :] = out[:, :LANES]
        scratch[:, p + 1, :] = out[:, LANES:]
    per_row = LANES // (2 * rows)
    x_row = wx[pl.ds(c // per_row, 1), :]
    first = (c % per_row) * (2 * rows)
    east = jnp.where(upper, column_of(x_row, first + rows, rows, lane), column_of(x_row, first, rows, lane))
    y_row = wy[pl.ds(r // 2, 1), :]
    y_row = jnp.broadcast_to(y_row, shape)
    north = jnp.where(upper == (r % 2 == 1), y_row, pltpu.roll(y_row, HALF, 1))
    weight = east * north
    field = scratch[...]
    modal[...] = field.astype(BF16)
    send[...] = (field * weight[None]).astype(BF16)


def scatter_blocks(wide, out):
    n = wide.shape[0] // 2
    for b in range(wide.shape[1] // LANES):
        top = wide[:n, b * LANES : (b + 1) * LANES]
        low = wide[n:, b * LANES : (b + 1) * LANES]
        out[2 * b] = jnp.concatenate([top[:, :HALF], low[:, :HALF]], axis=1)
        out[2 * b + 1] = jnp.concatenate([top[:, HALF:], low[:, HALF:]], axis=1)


def to_east(got, basis, out):
    wide = dot(unfold(got[...]), basis[...], 0, 0).astype(BF16)
    scatter_blocks(wide, out)


def solve(coupling, got, basis, east, north, out, scaled):
    r = lax.axis_index("row")
    c = lax.axis_index("col")
    gravity = coupling[c]
    mine = unfold(got[...])
    spectral = dot(mine, basis[...], 0, 0)
    n = spectral.shape[0]
    lane = lax.broadcasted_iota(jnp.int32, (n, LANES), 1)
    roots = column_of(east[pl.ds(r // 2, 1), :], (r % 2) * HALF, n, lane)
    for b in range(spectral.shape[1] // LANES):
        divisor = 1.0 + gravity * (roots + north[b : b + 1, :])
        scaled[:, b * LANES : (b + 1) * LANES] = (spectral[:, b * LANES : (b + 1) * LANES] / divisor).astype(BF16)
    wide = dot(scaled[...], basis[...], 1, 1).astype(BF16)
    scatter_blocks(wide, out)


def from_east(got, basis, out):
    solved = dot(basis[...], unfold(got[...]), 1, 0).astype(BF16)
    rows = 2 * out.shape[1]
    for c in range(out.shape[0]):
        out[c] = fold(solved[c * rows : (c + 1) * rows])


def finish(got, modal, forcing, restore, out, difference, total):
    difference[...] = got[...].astype(F32) - modal[...].astype(F32)
    rows = difference.shape[1]
    left = left_terms(restore[...])
    for p in range(0, rows, 2):
        field = jnp.concatenate([difference[:, p, :], difference[:, p + 1, :]], axis=1)
        correction = dot(left, right_terms(field), 1, 0)
        total[:, p, :] = forcing[:, p, :] + correction[:, :LANES]
        total[:, p + 1, :] = forcing[:, p + 1, :] + correction[:, LANES:]
    for level in range(out.shape[0]):
        v = total[level].astype(BF16)
        out[level, :rows, :] = v[:, :HALF]
        out[level, rows:, :] = v[:, HALF:]


SMEM = pl.BlockSpec(memory_space=pltpu.SMEM)
VMEM = pl.BlockSpec(memory_space=pltpu.VMEM)


def call(body, smem, vmem, outs, scratch, *operands):
    return pl.pallas_call(
        body,
        in_specs=[SMEM] * smem + [VMEM] * vmem,
        out_specs=[VMEM] * len(outs),
        out_shape=[jax.ShapeDtypeStruct(shape, dtype) for shape, dtype in outs],
        scratch_shapes=[pltpu.VMEM(shape, dtype) for shape, dtype in scratch],
        compiler_params=pltpu.CompilerParams(vmem_limit_bytes=VMEM_LIMIT),
    )(*operands)


def exchange(v, axis):
    return lax.all_to_all(v, axis, split_axis=0, concat_axis=0, tiled=True)


def local(
    potential_temp,
    humidity,
    absorb,
    solar_flux,
    emission,
    sunlit,
    project,
    restore,
    east_basis,
    north_basis,
    east_weight,
    north_weight,
    east_eigen,
    north_eigen,
    coupling,
):
    levels, east_local, north_local = potential_temp.shape
    modes = project.shape[0]
    rows = east_local // 2
    n_row = north_basis.shape[0] // north_local
    tile = (rows, LANES)
    block = (HALF // 2, LANES)
    lanes = lambda v: v.reshape(-1, LANES)
    forcing, send, modal = call(
        physics,
        4,
        5,
        [((levels, *tile), F32), ((modes, *tile), BF16), ((modes, *tile), BF16)],
        [((modes, *tile), F32)],
        absorb,
        solar_flux,
        emission,
        sunlit,
        potential_temp,
        humidity,
        project,
        lanes(east_weight),
        lanes(north_weight),
    )
    (send,) = call(to_east, 0, 2, [((n_row, *block), BF16)], [], exchange(send, "col"), east_basis)
    (send,) = call(
        solve,
        1,
        4,
        [((n_row, *block), BF16)],
        [((HALF, north_basis.shape[0]), BF16)],
        coupling,
        exchange(send, "row"),
        north_basis,
        lanes(east_eigen),
        lanes(north_eigen),
    )
    (send,) = call(from_east, 0, 2, [((modes, *tile), BF16)], [], exchange(send, "row"), east_basis)
    (out,) = call(
        finish,
        0,
        4,
        [((levels, east_local, north_local), BF16)],
        [((modes, *tile), F32), ((levels, *tile), F32)],
        exchange(send, "col"),
        modal,
        forcing,
        restore,
    )
    return out


def solution(mesh):
    spread = P(None, "col", "row")
    in_specs = (spread, spread) + (P(),) * 13
    return jax.shard_map(local, mesh=mesh, in_specs=in_specs, out_specs=spread, check_vma=False)
```

```python
import jax
import jax.numpy as jnp
from jax import lax
from jax.experimental import pallas as pl
from jax.experimental.pallas import tpu as pltpu
from jax.sharding import PartitionSpec as P

F32 = jnp.float32
BF16 = jnp.bfloat16
HALF = 64
LANES = 128
GROUPS = 4
COST = 4_000_000_000
VMEM_LIMIT = 12 * 1024 * 1024


def dot(a, b, da, db):
    return lax.dot_general(a, b, (((da,), (db,)), ((), ())), preferred_element_type=F32)


def fold(v):
    n = v.shape[0] // 2
    return jnp.concatenate([v[:n], v[n:]], axis=1)


def unfold(v):
    k, n, _ = v.shape
    return jnp.concatenate([v[:, :, :HALF], v[:, :, HALF:]], axis=1).reshape(k * 2 * n, HALF)


def halves(v):
    high = v.astype(BF16)
    return high, (v - high.astype(F32)).astype(BF16)


def left_terms(v):
    high, low = halves(v)
    return jnp.concatenate([high, low, high], axis=1)


def right_terms(v):
    high, low = halves(v)
    return jnp.concatenate([high, high, low], axis=0)


def column_of(row, first, rows, lane):
    place = lax.broadcasted_iota(jnp.int32, (rows, LANES), 0) + first
    return jnp.sum(jnp.where(lane == place, jnp.broadcast_to(row, (rows, LANES)), 0.0), axis=1, keepdims=True)


def physics(*refs):
    sources = refs[:9]
    forcing, send, modal = refs[9:12]
    absorb, flux, emission, sunlit, temp, vapour, project, wx, wy = refs[12:21]
    scratch, done = refs[21:]
    levels = temp.shape[0]
    bands = absorb.shape[0]
    rows = temp.shape[1] // 2
    group = levels // GROUPS
    cuts = [pl.ds(k * group, group) for k in range(GROUPS)]
    copy = pltpu.make_async_copy
    small = [
        copy(sources[k], refs[12 + k], done.at[k]) for k in (0, 1, 2, 3, 6, 7, 8)
    ]
    large = [
        [
            copy(sources[k].at[cut], refs[12 + k].at[cut], done.at[9 + 2 * n + k - 4])
            for k in (4, 5)
        ]
        for n, cut in enumerate(cuts)
    ]
    for item in small[:4] + [item for pair in large for item in pair] + small[4:]:
        item.start()
    for item in small[:4]:
        item.wait()
    r = lax.axis_index("row")
    c = lax.axis_index("col")
    shape = (rows, LANES)
    lane = lax.broadcasted_iota(jnp.int32, shape, 1)
    upper = lane >= HALF
    number = lax.broadcasted_iota(jnp.int32, shape, 0) * HALF + lane + jnp.where(upper, rows * HALF - HALF, 0)
    lit = (number < sunlit[r, c]).astype(F32)
    through = [lit * flux[b] for b in range(bands)]
    before = through[0] + through[1] + through[2] + through[3]
    emitted = emission[0] + emission[1] + emission[2] + emission[3]
    for level in range(levels):
        if level % group == 0:
            for item in large[level // group]:
                item.wait()
        t = fold(temp[level]).astype(F32)
        h = fold(vapour[level]).astype(F32)
        kept = None
        after = None
        for b in range(bands):
            pass_through = jnp.exp(h * (-absorb[b, level]))
            through[b] = through[b] * pass_through
            part = pass_through * emission[b]
            kept = part if kept is None else kept + part
            after = through[b] if after is None else after + through[b]
        forcing[level] = t + (before - after) - (emitted - kept) * t
        before = after
    for item in small[4:]:
        item.wait()
    left = left_terms(project[...])
    for p in range(0, rows, 2):
        field = jnp.concatenate([forcing[:, p, :], forcing[:, p + 1, :]], axis=1)
        out = dot(left, right_terms(field), 1, 0)
        scratch[:, p, :] = out[:, :LANES]
        scratch[:, p + 1, :] = out[:, LANES:]
    per_row = LANES // (2 * rows)
    x_row = wx[pl.ds(c // per_row, 1), :]
    first = (c % per_row) * (2 * rows)
    east = jnp.where(upper, column_of(x_row, first + rows, rows, lane), column_of(x_row, first, rows, lane))
    y_row = wy[pl.ds(r // 2, 1), :]
    y_row = jnp.broadcast_to(y_row, shape)
    north = jnp.where(upper == (r % 2 == 1), y_row, pltpu.roll(y_row, HALF, 1))
    weight = east * north
    field = scratch[...]
    modal[...] = field.astype(BF16)
    send[...] = (field * weight[None]).astype(BF16)


def scatter_blocks(wide, out):
    n = wide.shape[0] // 2
    for b in range(wide.shape[1] // LANES):
        top = wide[:n, b * LANES : (b + 1) * LANES]
        low = wide[n:, b * LANES : (b + 1) * LANES]
        out[2 * b] = jnp.concatenate([top[:, :HALF], low[:, :HALF]], axis=1)
        out[2 * b + 1] = jnp.concatenate([top[:, HALF:], low[:, HALF:]], axis=1)


def to_east(got, basis, out):
    wide = dot(unfold(got[...]), basis[...], 0, 0).astype(BF16)
    scatter_blocks(wide, out)


def solve(coupling, got, basis, east, north, out, scaled):
    r = lax.axis_index("row")
    c = lax.axis_index("col")
    gravity = coupling[c]
    mine = unfold(got[...])
    spectral = dot(mine, basis[...], 0, 0)
    n = spectral.shape[0]
    lane = lax.broadcasted_iota(jnp.int32, (n, LANES), 1)
    roots = column_of(east[pl.ds(r // 2, 1), :], (r % 2) * HALF, n, lane)
    for b in range(spectral.shape[1] // LANES):
        divisor = 1.0 + gravity * (roots + north[b : b + 1, :])
        scaled[:, b * LANES : (b + 1) * LANES] = (spectral[:, b * LANES : (b + 1) * LANES] / divisor).astype(BF16)
    wide = dot(scaled[...], basis[...], 1, 1).astype(BF16)
    scatter_blocks(wide, out)


def from_east(got, basis, out):
    solved = dot(basis[...], unfold(got[...]), 1, 0).astype(BF16)
    rows = 2 * out.shape[1]
    for c in range(out.shape[0]):
        out[c] = fold(solved[c * rows : (c + 1) * rows])


def finish(got, modal, forcing, restore, target, out, difference, total, done):
    difference[...] = got[...].astype(F32) - modal[...].astype(F32)
    rows = difference.shape[1]
    left = left_terms(restore[...])
    for p in range(0, rows, 2):
        field = jnp.concatenate([difference[:, p, :], difference[:, p + 1, :]], axis=1)
        correction = dot(left, right_terms(field), 1, 0)
        total[:, p, :] = forcing[:, p, :] + correction[:, :LANES]
        total[:, p + 1, :] = forcing[:, p + 1, :] + correction[:, LANES:]
    group = out.shape[0] // GROUPS
    copies = []
    for k in range(GROUPS):
        cut = pl.ds(k * group, group)
        for level in range(k * group, (k + 1) * group):
            v = total[level].astype(BF16)
            out[level, :rows, :] = v[:, :HALF]
            out[level, rows:, :] = v[:, HALF:]
        copies.append(pltpu.make_async_copy(out.at[cut], target.at[cut], done.at[k]))
        copies[k].start()
    for item in copies:
        item.wait()


SMEM = pl.BlockSpec(memory_space=pltpu.SMEM)
VMEM = pl.BlockSpec(memory_space=pltpu.VMEM)
HBM = pl.BlockSpec(memory_space=pltpu.HBM)


def call(body, in_specs, out_specs, outs, scratch, *operands):
    return pl.pallas_call(
        body,
        in_specs=in_specs,
        out_specs=out_specs,
        out_shape=[jax.ShapeDtypeStruct(shape, dtype) for shape, dtype in outs],
        scratch_shapes=scratch,
        compiler_params=pltpu.CompilerParams(vmem_limit_bytes=VMEM_LIMIT),
        cost_estimate=pl.CostEstimate(flops=COST, bytes_accessed=COST // 1000, transcendentals=0),
    )(*operands)


def exchange(v, axis):
    return lax.all_to_all(v, axis, split_axis=0, concat_axis=0, tiled=True)


def local(
    potential_temp,
    humidity,
    absorb,
    solar_flux,
    emission,
    sunlit,
    project,
    restore,
    east_basis,
    north_basis,
    east_weight,
    north_weight,
    east_eigen,
    north_eigen,
    coupling,
):
    levels, east_local, north_local = potential_temp.shape
    modes = project.shape[0]
    rows = east_local // 2
    n_row = north_basis.shape[0] // north_local
    tile = (rows, LANES)
    block = (HALF // 2, LANES)
    lanes = lambda v: v.reshape(-1, LANES)
    sources = (
        absorb,
        solar_flux,
        emission,
        sunlit,
        potential_temp,
        humidity,
        project,
        lanes(east_weight),
        lanes(north_weight),
    )
    held = [pltpu.SMEM] * 4 + [pltpu.VMEM] * 5
    forcing, send, modal = call(
        physics,
        [HBM] * 9,
        [VMEM] * 3,
        [((levels, *tile), F32), ((modes, *tile), BF16), ((modes, *tile), BF16)],
        [space(v.shape, v.dtype) for space, v in zip(held, sources)]
        + [pltpu.VMEM((modes, *tile), F32), pltpu.SemaphoreType.DMA((9 + 2 * GROUPS,))],
        *(pltpu.with_memory_space_constraint(v, pltpu.HBM) for v in sources),
    )
    (send,) = call(
        to_east, [VMEM] * 2, [VMEM], [((n_row, *block), BF16)], [], exchange(send, "col"), east_basis
    )
    (send,) = call(
        solve,
        [SMEM] + [VMEM] * 4,
        [VMEM],
        [((n_row, *block), BF16)],
        [pltpu.VMEM((HALF, north_basis.shape[0]), BF16)],
        coupling,
        exchange(send, "row"),
        north_basis,
        lanes(east_eigen),
        lanes(north_eigen),
    )
    (send,) = call(
        from_east, [VMEM] * 2, [VMEM], [((modes, *tile), BF16)], [], exchange(send, "row"), east_basis
    )
    shape = (levels, east_local, north_local)
    (out,) = call(
        finish,
        [VMEM] * 4,
        [HBM],
        [(shape, BF16)],
        [
            pltpu.VMEM(shape, BF16),
            pltpu.VMEM((modes, *tile), F32),
            pltpu.VMEM((levels, *tile), F32),
            pltpu.SemaphoreType.DMA((GROUPS,)),
        ],
        exchange(send, "col"),
        modal,
        forcing,
        restore,
    )
    return out


def solution(mesh):
    spread = P(None, "col", "row")
    in_specs = (spread, spread) + (P(),) * 13
    return jax.shard_map(local, mesh=mesh, in_specs=in_specs, out_specs=spread, check_vma=False)
```

```python
import jax
import jax.numpy as jnp
from jax import lax
from jax.experimental import pallas as pl
from jax.experimental.pallas import tpu as pltpu
from jax.sharding import PartitionSpec as P

F32 = jnp.float32
BF16 = jnp.bfloat16
HALF = 64
LANES = 128
GROUPS = 2
MINUS_LOG2_E = -1.4426950408889634
COST = 4_000_000_000
VMEM_LIMIT = 12 * 1024 * 1024


def dot(a, b, da, db):
    return lax.dot_general(a, b, (((da,), (db,)), ((), ())), preferred_element_type=F32)


def fold(v):
    n = v.shape[0] // 2
    return jnp.concatenate([v[:n], v[n:]], axis=1)


def unfold(v):
    k, n, _ = v.shape
    return jnp.concatenate([v[:, :, :HALF], v[:, :, HALF:]], axis=1).reshape(k * 2 * n, HALF)


def halves(v):
    high = v.astype(BF16)
    return high, (v - high.astype(F32)).astype(BF16)


def left_terms(v):
    high, low = halves(v)
    return jnp.concatenate([high, low, high], axis=1)


def right_terms(v):
    high, low = halves(v)
    return jnp.concatenate([high, high, low], axis=0)


def column_of(row, first, rows, lane):
    place = lax.broadcasted_iota(jnp.int32, (rows, LANES), 0) + first
    return jnp.sum(jnp.where(lane == place, jnp.broadcast_to(row, (rows, LANES)), 0.0), axis=1, keepdims=True)


def pair_of(ref, p, count, rows):
    return jnp.concatenate([ref[pl.ds(p + k, count, stride=rows), :] for k in (0, 1)], axis=1)


def set_pair(ref, p, value, rows):
    for k in (0, 1):
        ref[pl.ds(p + k, value.shape[0], stride=rows), :] = value[:, k * LANES : (k + 1) * LANES]


def physics(*refs):
    sources = refs[:9]
    forcing, send, modal = refs[9:12]
    absorb, flux, emission, sunlit, temp, vapour, project, wx, wy = refs[12:21]
    scratch, done = refs[21:]
    levels = temp.shape[0]
    bands = absorb.shape[0]
    rows = temp.shape[1] // 2
    group = levels // GROUPS
    cuts = [pl.ds(k * group, group) for k in range(GROUPS)]
    copy = pltpu.make_async_copy
    small = [
        copy(sources[k], refs[12 + k], done.at[k]) for k in (0, 1, 2, 3, 6, 7, 8)
    ]
    large = [
        [
            copy(sources[k].at[cut], refs[12 + k].at[cut], done.at[9 + 2 * n + k - 4])
            for k in (4, 5)
        ]
        for n, cut in enumerate(cuts)
    ]
    for item in small[:4] + [item for pair in large for item in pair] + small[4:]:
        item.start()
    for item in small[:4]:
        item.wait()
    r = lax.axis_index("row")
    c = lax.axis_index("col")
    shape = (rows, LANES)
    lane = lax.broadcasted_iota(jnp.int32, shape, 1)
    upper = lane >= HALF
    number = lax.broadcasted_iota(jnp.int32, shape, 0) * HALF + lane + jnp.where(upper, rows * HALF - HALF, 0)
    lit = (number < sunlit[r, c]).astype(F32)
    through = [lit * flux[b] for b in range(bands)]
    before = through[0] + through[1] + through[2] + through[3]
    emitted = emission[0] + emission[1] + emission[2] + emission[3]
    for level in range(levels):
        if level % group == 0:
            for item in large[level // group]:
                item.wait()
        t = fold(temp[level]).astype(F32)
        h = fold(vapour[level]).astype(F32) * MINUS_LOG2_E
        kept = None
        after = None
        for b in range(bands):
            pass_through = jnp.exp2(h * absorb[b, level])
            through[b] = through[b] * pass_through
            part = pass_through * emission[b]
            kept = part if kept is None else kept + part
            after = through[b] if after is None else after + through[b]
        forcing[level * rows : (level + 1) * rows, :] = t + (before - after) - (emitted - kept) * t
        before = after
    for item in small[4:]:
        item.wait()
    left = left_terms(project[...])
    for p in range(0, rows, 2):
        out = dot(left, right_terms(pair_of(forcing, p, levels, rows)), 1, 0)
        set_pair(scratch, p, out, rows)
    per_row = LANES // (2 * rows)
    x_row = wx[pl.ds(c // per_row, 1), :]
    first = (c % per_row) * (2 * rows)
    east = jnp.where(upper, column_of(x_row, first + rows, rows, lane), column_of(x_row, first, rows, lane))
    y_row = wy[pl.ds(r // 2, 1), :]
    y_row = jnp.broadcast_to(y_row, shape)
    north = jnp.where(upper == (r % 2 == 1), y_row, pltpu.roll(y_row, HALF, 1))
    weight = east * north
    field = scratch[...].reshape(modal.shape)
    modal[...] = field.astype(BF16)
    send[...] = (field * weight[None]).astype(BF16)


def scatter_blocks(wide, out):
    n = wide.shape[0] // 2
    for b in range(wide.shape[1] // LANES):
        top = wide[:n, b * LANES : (b + 1) * LANES]
        low = wide[n:, b * LANES : (b + 1) * LANES]
        out[2 * b] = jnp.concatenate([top[:, :HALF], low[:, :HALF]], axis=1)
        out[2 * b + 1] = jnp.concatenate([top[:, HALF:], low[:, HALF:]], axis=1)


def gather_blocks(got, wide):
    n = got.shape[1]
    for b in range(got.shape[0] // 2):
        one, two = got[2 * b], got[2 * b + 1]
        place = slice(b * LANES, (b + 1) * LANES)
        wide[:n, place] = jnp.concatenate([one[:, :HALF], two[:, :HALF]], axis=1)
        wide[n:, place] = jnp.concatenate([one[:, HALF:], two[:, HALF:]], axis=1)


def to_east(got, basis, out):
    wide = dot(unfold(got[...]), basis[...], 0, 0).astype(BF16)
    scatter_blocks(wide, out)


def solve(coupling, got, basis, east, north, out, scaled):
    r = lax.axis_index("row")
    c = lax.axis_index("col")
    place = lax.broadcasted_iota(jnp.int32, coupling.shape, 1)
    gravity = jnp.sum(jnp.where(place == c, coupling[...], 0.0), axis=1, keepdims=True)
    mine = unfold(got[...])
    spectral = dot(mine, basis[...], 0, 0)
    n = spectral.shape[0]
    lane = lax.broadcasted_iota(jnp.int32, (n, LANES), 1)
    roots = column_of(east[pl.ds(r // 2, 1), :], (r % 2) * HALF, n, lane)
    for b in range(spectral.shape[1] // LANES):
        divisor = 1.0 + gravity * (roots + north[b : b + 1, :])
        scaled[:, b * LANES : (b + 1) * LANES] = (spectral[:, b * LANES : (b + 1) * LANES] / divisor).astype(BF16)
    tall = dot(basis[...], scaled[...], 1, 1).astype(BF16)
    for b in range(out.shape[0]):
        out[b] = fold(tall[b * HALF : (b + 1) * HALF])


def from_east(got, basis, out, wide):
    gather_blocks(got, wide)
    solved = dot(basis[...], wide[...], 1, 1).astype(BF16)
    rows = 2 * out.shape[1]
    for c in range(out.shape[0]):
        out[c] = fold(solved[c * rows : (c + 1) * rows])


def finish(got, modal, forcing, restore, target, out, difference, total, done):
    modes, rows, _ = got.shape
    levels = out.shape[0]
    gap = got[...].astype(F32) - modal[...].astype(F32)
    difference[...] = gap.reshape(difference.shape)
    high, low = halves(restore[...])
    left = jnp.concatenate([high, low, high], axis=0)
    for p in range(0, rows, 2):
        correction = dot(left, right_terms(pair_of(difference, p, modes, rows)), 0, 0)
        set_pair(total, p, correction, rows)
    group = levels // GROUPS
    copies = []
    for k in range(GROUPS):
        cut = pl.ds(k * group, group)
        for level in range(k * group, (k + 1) * group):
            here = slice(level * rows, (level + 1) * rows)
            v = (forcing[here, :] + total[here, :]).astype(BF16)
            out[level, :rows, :] = v[:, :HALF]
            out[level, rows:, :] = v[:, HALF:]
        copies.append(pltpu.make_async_copy(out.at[cut], target.at[cut], done.at[k]))
        copies[k].start()
    for item in copies:
        item.wait()


SMEM = pl.BlockSpec(memory_space=pltpu.SMEM)
VMEM = pl.BlockSpec(memory_space=pltpu.VMEM)
HBM = pl.BlockSpec(memory_space=pltpu.HBM)


def call(body, in_specs, out_specs, outs, scratch, *operands):
    return pl.pallas_call(
        body,
        in_specs=in_specs,
        out_specs=out_specs,
        out_shape=[jax.ShapeDtypeStruct(shape, dtype) for shape, dtype in outs],
        scratch_shapes=scratch,
        compiler_params=pltpu.CompilerParams(vmem_limit_bytes=VMEM_LIMIT),
        cost_estimate=pl.CostEstimate(flops=COST, bytes_accessed=COST // 1000, transcendentals=0),
    )(*operands)


def exchange(v, axis):
    return lax.all_to_all(v, axis, split_axis=0, concat_axis=0, tiled=True)


def local(
    potential_temp,
    humidity,
    absorb,
    solar_flux,
    emission,
    sunlit,
    project,
    restore,
    east_basis,
    north_basis,
    east_weight,
    north_weight,
    east_eigen,
    north_eigen,
    coupling,
):
    levels, east_local, north_local = potential_temp.shape
    modes = project.shape[0]
    rows = east_local // 2
    n_row = north_basis.shape[0] // north_local
    tile = (rows, LANES)
    block = (HALF // 2, LANES)
    lanes = lambda v: v.reshape(-1, LANES)
    sources = (
        absorb,
        solar_flux,
        emission,
        sunlit,
        potential_temp,
        humidity,
        project,
        lanes(east_weight),
        lanes(north_weight),
    )
    held = [pltpu.SMEM] * 4 + [pltpu.VMEM] * 5
    forcing, send, modal = call(
        physics,
        [HBM] * 9,
        [VMEM] * 3,
        [((levels * rows, LANES), F32), ((modes, *tile), BF16), ((modes, *tile), BF16)],
        [space(v.shape, v.dtype) for space, v in zip(held, sources)]
        + [pltpu.VMEM((modes * rows, LANES), F32), pltpu.SemaphoreType.DMA((9 + 2 * GROUPS,))],
        *(pltpu.with_memory_space_constraint(v, pltpu.HBM) for v in sources),
    )
    (send,) = call(
        to_east, [VMEM] * 2, [VMEM], [((n_row, *block), BF16)], [], exchange(send, "col"), east_basis
    )
    (send,) = call(
        solve,
        [VMEM] * 5,
        [VMEM],
        [((n_row, *block), BF16)],
        [pltpu.VMEM((HALF, north_basis.shape[0]), BF16)],
        coupling.reshape(1, -1),
        exchange(send, "row"),
        north_basis,
        lanes(east_eigen),
        lanes(north_eigen),
    )
    (send,) = call(
        from_east,
        [VMEM] * 2,
        [VMEM],
        [((modes, *tile), BF16)],
        [pltpu.VMEM((HALF, east_basis.shape[0]), BF16)],
        exchange(send, "row"),
        east_basis,
    )
    shape = (levels, east_local, north_local)
    (out,) = call(
        finish,
        [VMEM] * 4,
        [HBM],
        [(shape, BF16)],
        [
            pltpu.VMEM(shape, BF16),
            pltpu.VMEM((modes * rows, LANES), F32),
            pltpu.VMEM((levels * rows, LANES), F32),
            pltpu.SemaphoreType.DMA((GROUPS,)),
        ],
        exchange(send, "col"),
        modal,
        forcing,
        restore.T,
    )
    return out


def solution(mesh):
    spread = P(None, "col", "row")
    in_specs = (spread, spread) + (P(),) * 13
    return jax.shard_map(local, mesh=mesh, in_specs=in_specs, out_specs=spread, check_vma=False)
```

```python
import jax
import jax.numpy as jnp
from jax import lax
from jax.experimental import pallas as pl
from jax.experimental.pallas import tpu as pltpu
from jax.sharding import PartitionSpec as P

F32 = jnp.float32
BF16 = jnp.bfloat16
HALF = 64
LANES = 128
GROUPS = 2
MINUS_LOG2_E = -1.4426950408889634
COL_MASK = 21
ROW_MASK = 6
COST = 4_000_000_000
VMEM_LIMIT = 12 * 1024 * 1024


def dot(a, b, da, db):
    return lax.dot_general(a, b, (((da,), (db,)), ((), ())), preferred_element_type=F32)


def fold(v):
    n = v.shape[0] // 2
    return jnp.concatenate([v[:n], v[n:]], axis=1)


def unfold(ref, mask):
    k, n, _ = ref.shape
    v = jnp.stack([ref[b ^ mask] for b in range(k)], axis=0)
    return jnp.concatenate([v[:, :, :HALF], v[:, :, HALF:]], axis=1).reshape(k * 2 * n, HALF)


def halves(v):
    high = v.astype(BF16)
    return high, (v - high.astype(F32)).astype(BF16)


def left_terms(v):
    high, low = halves(v)
    return jnp.concatenate([high, low, high], axis=1)


def right_terms(v):
    high, low = halves(v)
    return jnp.concatenate([high, high, low], axis=0)


def column_of(row, first, rows, lane):
    place = lax.broadcasted_iota(jnp.int32, (rows, LANES), 0) + first
    return jnp.sum(jnp.where(lane == place, jnp.broadcast_to(row, (rows, LANES)), 0.0), axis=1, keepdims=True)


def pair_of(ref, p, count, rows):
    return jnp.concatenate([ref[pl.ds(p + k, count, stride=rows), :] for k in (0, 1)], axis=1)


def set_pair(ref, p, value, rows):
    for k in (0, 1):
        ref[pl.ds(p + k, value.shape[0], stride=rows), :] = value[:, k * LANES : (k + 1) * LANES]


def physics(*refs):
    sources = refs[:9]
    forcing, send, modal = refs[9:12]
    absorb, flux, emission, sunlit, temp, vapour, project, wx, wy = refs[12:21]
    scratch, done = refs[21:]
    levels = temp.shape[0]
    bands = absorb.shape[0]
    rows = temp.shape[1] // 2
    group = levels // GROUPS
    cuts = [pl.ds(k * group, group) for k in range(GROUPS)]
    copy = pltpu.make_async_copy
    small = [
        copy(sources[k], refs[12 + k], done.at[k]) for k in (0, 1, 2, 3, 6, 7, 8)
    ]
    large = [
        [
            copy(sources[k].at[cut], refs[12 + k].at[cut], done.at[9 + 2 * n + k - 4])
            for k in (4, 5)
        ]
        for n, cut in enumerate(cuts)
    ]
    for item in small[:4] + [item for pair in large for item in pair] + small[4:]:
        item.start()
    for item in small[:4]:
        item.wait()
    r = lax.axis_index("row")
    c = lax.axis_index("col")
    shape = (rows, LANES)
    lane = lax.broadcasted_iota(jnp.int32, shape, 1)
    upper = lane >= HALF
    number = lax.broadcasted_iota(jnp.int32, shape, 0) * HALF + lane + jnp.where(upper, rows * HALF - HALF, 0)
    lit = (number < sunlit[r, c]).astype(F32)
    through = [lit * flux[b] for b in range(bands)]
    before = through[0] + through[1] + through[2] + through[3]
    emitted = emission[0] + emission[1] + emission[2] + emission[3]
    for level in range(levels):
        if level % group == 0:
            for item in large[level // group]:
                item.wait()
        t = fold(temp[level]).astype(F32)
        h = fold(vapour[level]).astype(F32) * MINUS_LOG2_E
        kept = None
        after = None
        for b in range(bands):
            pass_through = jnp.exp2(h * absorb[b, level])
            through[b] = through[b] * pass_through
            part = pass_through * emission[b]
            kept = part if kept is None else kept + part
            after = through[b] if after is None else after + through[b]
        forcing[level * rows : (level + 1) * rows, :] = t + (before - after) - (emitted - kept) * t
        before = after
    for item in small[4:]:
        item.wait()
    left = left_terms(project[...])
    for p in range(0, rows, 2):
        out = dot(left, right_terms(pair_of(forcing, p, levels, rows)), 1, 0)
        set_pair(scratch, p, out, rows)
    per_row = LANES // (2 * rows)
    x_row = wx[pl.ds(c // per_row, 1), :]
    first = (c % per_row) * (2 * rows)
    east = jnp.where(upper, column_of(x_row, first + rows, rows, lane), column_of(x_row, first, rows, lane))
    y_row = wy[pl.ds(r // 2, 1), :]
    y_row = jnp.broadcast_to(y_row, shape)
    north = jnp.where(upper == (r % 2 == 1), y_row, pltpu.roll(y_row, HALF, 1))
    weight = east * north
    field = scratch[...].reshape(modal.shape)
    modal[...] = field.astype(BF16)
    send[...] = (field * weight[None]).astype(BF16)


def scatter_blocks(wide, out):
    n = wide.shape[0] // 2
    for b in range(wide.shape[1] // LANES):
        top = wide[:n, b * LANES : (b + 1) * LANES]
        low = wide[n:, b * LANES : (b + 1) * LANES]
        out[2 * b] = jnp.concatenate([top[:, :HALF], low[:, :HALF]], axis=1)
        out[2 * b + 1] = jnp.concatenate([top[:, HALF:], low[:, HALF:]], axis=1)


def gather_blocks(got, wide):
    n = got.shape[1]
    for b in range(got.shape[0] // 2):
        one, two = got[2 * b], got[2 * b + 1]
        place = slice(b * LANES, (b + 1) * LANES)
        wide[:n, place] = jnp.concatenate([one[:, :HALF], two[:, :HALF]], axis=1)
        wide[n:, place] = jnp.concatenate([one[:, HALF:], two[:, HALF:]], axis=1)


def to_east(got, basis, out):
    wide = dot(unfold(got, COL_MASK), basis[...], 0, 0).astype(BF16)
    scatter_blocks(wide, out)


def solve(coupling, got, basis, east, north, out, scaled):
    r = lax.axis_index("row") ^ ROW_MASK
    c = lax.axis_index("col") ^ COL_MASK
    place = lax.broadcasted_iota(jnp.int32, coupling.shape, 1)
    gravity = jnp.sum(jnp.where(place == c, coupling[...], 0.0), axis=1, keepdims=True)
    mine = unfold(got, ROW_MASK)
    spectral = dot(mine, basis[...], 0, 0)
    n = spectral.shape[0]
    lane = lax.broadcasted_iota(jnp.int32, (n, LANES), 1)
    roots = column_of(east[pl.ds(r // 2, 1), :], (r % 2) * HALF, n, lane)
    for b in range(spectral.shape[1] // LANES):
        divisor = 1.0 + gravity * (roots + north[b : b + 1, :])
        scaled[:, b * LANES : (b + 1) * LANES] = (spectral[:, b * LANES : (b + 1) * LANES] / divisor).astype(BF16)
    tall = dot(basis[...], scaled[...], 1, 1).astype(BF16)
    for b in range(out.shape[0]):
        out[b ^ ROW_MASK] = fold(tall[b * HALF : (b + 1) * HALF])


def from_east(got, basis, out, wide):
    gather_blocks(got, wide)
    solved = dot(basis[...], wide[...], 1, 1).astype(BF16)
    rows = 2 * out.shape[1]
    for c in range(out.shape[0]):
        out[c ^ COL_MASK] = fold(solved[c * rows : (c + 1) * rows])


def finish(got, modal, forcing, restore, target, out, difference, total, done):
    modes, rows, _ = got.shape
    levels = out.shape[0]
    gap = got[...].astype(F32) - modal[...].astype(F32)
    difference[...] = gap.reshape(difference.shape)
    high, low = halves(restore[...])
    left = jnp.concatenate([high, low, high], axis=0)
    for p in range(0, rows, 2):
        correction = dot(left, right_terms(pair_of(difference, p, modes, rows)), 0, 0)
        set_pair(total, p, correction, rows)
    group = levels // GROUPS
    copies = []
    for k in range(GROUPS):
        cut = pl.ds(k * group, group)
        for level in range(k * group, (k + 1) * group):
            here = slice(level * rows, (level + 1) * rows)
            v = (forcing[here, :] + total[here, :]).astype(BF16)
            out[level, :rows, :] = v[:, :HALF]
            out[level, rows:, :] = v[:, HALF:]
        copies.append(pltpu.make_async_copy(out.at[cut], target.at[cut], done.at[k]))
        copies[k].start()
    for item in copies:
        item.wait()


SMEM = pl.BlockSpec(memory_space=pltpu.SMEM)
VMEM = pl.BlockSpec(memory_space=pltpu.VMEM)
HBM = pl.BlockSpec(memory_space=pltpu.HBM)


def call(body, in_specs, out_specs, outs, scratch, *operands):
    return pl.pallas_call(
        body,
        in_specs=in_specs,
        out_specs=out_specs,
        out_shape=[jax.ShapeDtypeStruct(shape, dtype) for shape, dtype in outs],
        scratch_shapes=scratch,
        compiler_params=pltpu.CompilerParams(vmem_limit_bytes=VMEM_LIMIT),
        cost_estimate=pl.CostEstimate(flops=COST, bytes_accessed=COST // 1000, transcendentals=0),
    )(*operands)


def exchange(v, axis):
    mask = COL_MASK if axis == "col" else ROW_MASK
    order = [k ^ mask for k in range(v.shape[0])]
    return lax.all_to_all(v, axis, split_axis=0, concat_axis=0, tiled=True, axis_index_groups=[order])


def local(
    potential_temp,
    humidity,
    absorb,
    solar_flux,
    emission,
    sunlit,
    project,
    restore,
    east_basis,
    north_basis,
    east_weight,
    north_weight,
    east_eigen,
    north_eigen,
    coupling,
):
    levels, east_local, north_local = potential_temp.shape
    modes = project.shape[0]
    rows = east_local // 2
    n_row = north_basis.shape[0] // north_local
    tile = (rows, LANES)
    block = (HALF // 2, LANES)
    lanes = lambda v: v.reshape(-1, LANES)
    sources = (
        absorb,
        solar_flux,
        emission,
        sunlit,
        potential_temp,
        humidity,
        project,
        lanes(east_weight),
        lanes(north_weight),
    )
    held = [pltpu.SMEM] * 4 + [pltpu.VMEM] * 5
    forcing, send, modal = call(
        physics,
        [HBM] * 9,
        [VMEM] * 3,
        [((levels * rows, LANES), F32), ((modes, *tile), BF16), ((modes, *tile), BF16)],
        [space(v.shape, v.dtype) for space, v in zip(held, sources)]
        + [pltpu.VMEM((modes * rows, LANES), F32), pltpu.SemaphoreType.DMA((9 + 2 * GROUPS,))],
        *(pltpu.with_memory_space_constraint(v, pltpu.HBM) for v in sources),
    )
    (send,) = call(
        to_east, [VMEM] * 2, [VMEM], [((n_row, *block), BF16)], [], exchange(send, "col"), east_basis
    )
    (send,) = call(
        solve,
        [VMEM] * 5,
        [VMEM],
        [((n_row, *block), BF16)],
        [pltpu.VMEM((HALF, north_basis.shape[0]), BF16)],
        coupling.reshape(1, -1),
        exchange(send, "row"),
        north_basis,
        lanes(east_eigen),
        lanes(north_eigen),
    )
    (send,) = call(
        from_east,
        [VMEM] * 2,
        [VMEM],
        [((modes, *tile), BF16)],
        [pltpu.VMEM((HALF, east_basis.shape[0]), BF16)],
        exchange(send, "row"),
        east_basis,
    )
    shape = (levels, east_local, north_local)
    (out,) = call(
        finish,
        [VMEM] * 4,
        [HBM],
        [(shape, BF16)],
        [
            pltpu.VMEM(shape, BF16),
            pltpu.VMEM((modes * rows, LANES), F32),
            pltpu.VMEM((levels * rows, LANES), F32),
            pltpu.SemaphoreType.DMA((GROUPS,)),
        ],
        exchange(send, "col"),
        modal,
        forcing,
        restore.T,
    )
    return out


def solution(mesh):
    spread = P(None, "col", "row")
    in_specs = (spread, spread) + (P(),) * 13
    return jax.shard_map(local, mesh=mesh, in_specs=in_specs, out_specs=spread, check_vma=False)
```

```python
import jax
import jax.numpy as jnp
from jax import lax
from jax.experimental import pallas as pl
from jax.experimental.pallas import tpu as pltpu
from jax.sharding import PartitionSpec as P

F32 = jnp.float32
BF16 = jnp.bfloat16
HALF = 64
LANES = 128
GROUPS = 2
OUT_GROUPS = 4
MINUS_LOG2_E = -1.4426950408889634
COL_MASK = 21
ROW_MASK = 6
COST = 4_000_000_000
VMEM_LIMIT = 12 * 1024 * 1024


def dot(a, b, da, db):
    return lax.dot_general(a, b, (((da,), (db,)), ((), ())), preferred_element_type=F32)


def fold(v):
    n = v.shape[0] // 2
    return jnp.concatenate([v[:n], v[n:]], axis=1)


def unfold(ref, mask):
    k, n, _ = ref.shape
    v = jnp.stack([ref[b ^ mask] for b in range(k)], axis=0)
    return jnp.concatenate([v[:, :, :HALF], v[:, :, HALF:]], axis=1).reshape(k * 2 * n, HALF)


def halves(v):
    high = v.astype(BF16)
    return high, (v - high.astype(F32)).astype(BF16)


def left_terms(v):
    high, low = halves(v)
    return jnp.concatenate([high, low, high], axis=1)


def right_terms(v):
    high, low = halves(v)
    return jnp.concatenate([high, high, low], axis=0)


def column_of(row, first, rows, lane):
    place = lax.broadcasted_iota(jnp.int32, (rows, LANES), 0) + first
    return jnp.sum(jnp.where(lane == place, jnp.broadcast_to(row, (rows, LANES)), 0.0), axis=1, keepdims=True)


def pair_of(ref, p, count, rows):
    return jnp.concatenate([ref[pl.ds(p + k, count, stride=rows), :] for k in (0, 1)], axis=1)


def set_pair(ref, p, value, rows):
    for k in (0, 1):
        ref[pl.ds(p + k, value.shape[0], stride=rows), :] = value[:, k * LANES : (k + 1) * LANES]


def physics(*refs):
    sources = refs[:9]
    forcing, send, modal = refs[9:12]
    absorb, flux, emission, sunlit, temp, vapour, project, wx, wy = refs[12:21]
    scratch, done = refs[21:]
    levels = temp.shape[0]
    bands = absorb.shape[0]
    rows = temp.shape[1] // 2
    group = levels // GROUPS
    cuts = [pl.ds(k * group, group) for k in range(GROUPS)]
    copy = pltpu.make_async_copy
    small = [
        copy(sources[k], refs[12 + k], done.at[k]) for k in (0, 1, 2, 3, 6, 7, 8)
    ]
    large = [
        [
            copy(sources[k].at[cut], refs[12 + k].at[cut], done.at[9 + 2 * n + k - 4])
            for k in (4, 5)
        ]
        for n, cut in enumerate(cuts)
    ]
    for item in small[:4] + [item for pair in large for item in pair] + small[4:]:
        item.start()
    for item in small[:4]:
        item.wait()
    r = lax.axis_index("row")
    c = lax.axis_index("col")
    shape = (rows, LANES)
    lane = lax.broadcasted_iota(jnp.int32, shape, 1)
    upper = lane >= HALF
    number = lax.broadcasted_iota(jnp.int32, shape, 0) * HALF + lane + jnp.where(upper, rows * HALF - HALF, 0)
    lit = (number < sunlit[r, c]).astype(F32)
    through = [lit * flux[b] for b in range(bands)]
    before = through[0] + through[1] + through[2] + through[3]
    emitted = emission[0] + emission[1] + emission[2] + emission[3]
    for level in range(levels):
        if level % group == 0:
            for item in large[level // group]:
                item.wait()
        t = fold(temp[level]).astype(F32)
        h = fold(vapour[level]).astype(F32) * MINUS_LOG2_E
        kept = None
        after = None
        for b in range(bands):
            pass_through = jnp.exp2(h * absorb[b, level])
            through[b] = through[b] * pass_through
            part = pass_through * emission[b]
            kept = part if kept is None else kept + part
            after = through[b] if after is None else after + through[b]
        forcing[level * rows : (level + 1) * rows, :] = t + (before - after) - (emitted - kept) * t
        before = after
    for item in small[4:]:
        item.wait()
    left = left_terms(project[...])
    for p in range(0, rows, 2):
        out = dot(left, right_terms(pair_of(forcing, p, levels, rows)), 1, 0)
        set_pair(scratch, p, out, rows)
    per_row = LANES // (2 * rows)
    x_row = wx[pl.ds(c // per_row, 1), :]
    first = (c % per_row) * (2 * rows)
    east = jnp.where(upper, column_of(x_row, first + rows, rows, lane), column_of(x_row, first, rows, lane))
    y_row = wy[pl.ds(r // 2, 1), :]
    y_row = jnp.broadcast_to(y_row, shape)
    north = jnp.where(upper == (r % 2 == 1), y_row, pltpu.roll(y_row, HALF, 1))
    weight = east * north
    field = scratch[...].reshape(modal.shape)
    modal[...] = field.astype(BF16)
    send[...] = (field * weight[None]).astype(BF16)


def scatter_blocks(wide, out):
    n = wide.shape[0] // 2
    for b in range(wide.shape[1] // LANES):
        top = wide[:n, b * LANES : (b + 1) * LANES]
        low = wide[n:, b * LANES : (b + 1) * LANES]
        out[2 * b] = jnp.concatenate([top[:, :HALF], low[:, :HALF]], axis=1)
        out[2 * b + 1] = jnp.concatenate([top[:, HALF:], low[:, HALF:]], axis=1)


def gather_blocks(got, wide):
    n = got.shape[1]
    for b in range(got.shape[0] // 2):
        one, two = got[2 * b], got[2 * b + 1]
        place = slice(b * LANES, (b + 1) * LANES)
        wide[:n, place] = jnp.concatenate([one[:, :HALF], two[:, :HALF]], axis=1)
        wide[n:, place] = jnp.concatenate([one[:, HALF:], two[:, HALF:]], axis=1)


def to_east(got, basis, out):
    wide = dot(unfold(got, COL_MASK), basis[...], 0, 0).astype(BF16)
    scatter_blocks(wide, out)


def solve(coupling, got, basis, east, north, out, scaled):
    r = lax.axis_index("row") ^ ROW_MASK
    c = lax.axis_index("col") ^ COL_MASK
    place = lax.broadcasted_iota(jnp.int32, coupling.shape, 1)
    gravity = jnp.sum(jnp.where(place == c, coupling[...], 0.0), axis=1, keepdims=True)
    mine = unfold(got, ROW_MASK)
    spectral = dot(mine, basis[...], 0, 0)
    n = spectral.shape[0]
    lane = lax.broadcasted_iota(jnp.int32, (n, LANES), 1)
    roots = column_of(east[pl.ds(r // 2, 1), :], (r % 2) * HALF, n, lane)
    for b in range(spectral.shape[1] // LANES):
        divisor = 1.0 + gravity * (roots + north[b : b + 1, :])
        scaled[:, b * LANES : (b + 1) * LANES] = (spectral[:, b * LANES : (b + 1) * LANES] / divisor).astype(BF16)
    tall = dot(basis[...], scaled[...], 1, 1).astype(BF16)
    for b in range(out.shape[0]):
        out[b ^ ROW_MASK] = fold(tall[b * HALF : (b + 1) * HALF])


def from_east(got, basis, out, wide):
    gather_blocks(got, wide)
    solved = dot(basis[...], wide[...], 1, 1).astype(BF16)
    rows = 2 * out.shape[1]
    for c in range(out.shape[0]):
        out[c ^ COL_MASK] = fold(solved[c * rows : (c + 1) * rows])


def finish(got, modal, forcing, restore, target, out, difference, total, done):
    modes, rows, _ = got.shape
    levels = out.shape[0]
    gap = got[...].astype(F32) - modal[...].astype(F32)
    difference[...] = gap.reshape(difference.shape)
    high, low = halves(restore[...])
    left = jnp.concatenate([high, low, high], axis=0)
    right = [right_terms(pair_of(difference, p, modes, rows)) for p in range(0, rows, 2)]
    group = levels // OUT_GROUPS
    copies = []
    for k in range(OUT_GROUPS):
        cut = pl.ds(k * group, group)
        for n in range(rows // 2):
            correction = dot(left[:, k * group : (k + 1) * group], right[n], 0, 0)
            for q in range(2):
                here = pl.ds(k * group * rows + 2 * n + q, group, stride=rows)
                total[here, :] = correction[:, q * LANES : (q + 1) * LANES]
        for level in range(k * group, (k + 1) * group):
            here = slice(level * rows, (level + 1) * rows)
            v = (forcing[here, :] + total[here, :]).astype(BF16)
            out[level, :rows, :] = v[:, :HALF]
            out[level, rows:, :] = v[:, HALF:]
        copies.append(pltpu.make_async_copy(out.at[cut], target.at[cut], done.at[k]))
        copies[k].start()
    for item in copies:
        item.wait()


SMEM = pl.BlockSpec(memory_space=pltpu.SMEM)
VMEM = pl.BlockSpec(memory_space=pltpu.VMEM)
HBM = pl.BlockSpec(memory_space=pltpu.HBM)


def call(body, in_specs, out_specs, outs, scratch, *operands):
    return pl.pallas_call(
        body,
        in_specs=in_specs,
        out_specs=out_specs,
        out_shape=[jax.ShapeDtypeStruct(shape, dtype) for shape, dtype in outs],
        scratch_shapes=scratch,
        compiler_params=pltpu.CompilerParams(vmem_limit_bytes=VMEM_LIMIT),
        cost_estimate=pl.CostEstimate(flops=COST, bytes_accessed=COST // 1000, transcendentals=0),
    )(*operands)


def exchange(v, axis):
    mask = COL_MASK if axis == "col" else ROW_MASK
    order = [k ^ mask for k in range(v.shape[0])]
    return lax.all_to_all(v, axis, split_axis=0, concat_axis=0, tiled=True, axis_index_groups=[order])


def local(
    potential_temp,
    humidity,
    absorb,
    solar_flux,
    emission,
    sunlit,
    project,
    restore,
    east_basis,
    north_basis,
    east_weight,
    north_weight,
    east_eigen,
    north_eigen,
    coupling,
):
    levels, east_local, north_local = potential_temp.shape
    modes = project.shape[0]
    rows = east_local // 2
    n_row = north_basis.shape[0] // north_local
    tile = (rows, LANES)
    block = (HALF // 2, LANES)
    lanes = lambda v: v.reshape(-1, LANES)
    sources = (
        absorb,
        solar_flux,
        emission,
        sunlit,
        potential_temp,
        humidity,
        project,
        lanes(east_weight),
        lanes(north_weight),
    )
    held = [pltpu.SMEM] * 4 + [pltpu.VMEM] * 5
    forcing, send, modal = call(
        physics,
        [HBM] * 9,
        [VMEM] * 3,
        [((levels * rows, LANES), F32), ((modes, *tile), BF16), ((modes, *tile), BF16)],
        [space(v.shape, v.dtype) for space, v in zip(held, sources)]
        + [pltpu.VMEM((modes * rows, LANES), F32), pltpu.SemaphoreType.DMA((9 + 2 * GROUPS,))],
        *(pltpu.with_memory_space_constraint(v, pltpu.HBM) for v in sources),
    )
    (send,) = call(
        to_east, [VMEM] * 2, [VMEM], [((n_row, *block), BF16)], [], exchange(send, "col"), east_basis
    )
    (send,) = call(
        solve,
        [VMEM] * 5,
        [VMEM],
        [((n_row, *block), BF16)],
        [pltpu.VMEM((HALF, north_basis.shape[0]), BF16)],
        coupling.reshape(1, -1),
        exchange(send, "row"),
        north_basis,
        lanes(east_eigen),
        lanes(north_eigen),
    )
    (send,) = call(
        from_east,
        [VMEM] * 2,
        [VMEM],
        [((modes, *tile), BF16)],
        [pltpu.VMEM((HALF, east_basis.shape[0]), BF16)],
        exchange(send, "row"),
        east_basis,
    )
    shape = (levels, east_local, north_local)
    (out,) = call(
        finish,
        [VMEM] * 4,
        [HBM],
        [(shape, BF16)],
        [
            pltpu.VMEM(shape, BF16),
            pltpu.VMEM((modes * rows, LANES), F32),
            pltpu.VMEM((levels * rows, LANES), F32),
            pltpu.SemaphoreType.DMA((OUT_GROUPS,)),
        ],
        exchange(send, "col"),
        modal,
        forcing,
        restore.T,
    )
    return out


def solution(mesh):
    spread = P(None, "col", "row")
    in_specs = (spread, spread) + (P(),) * 13
    return jax.shard_map(local, mesh=mesh, in_specs=in_specs, out_specs=spread, check_vma=False)
```
